32 devices in a mesh: dp: 8 (over y, x, core), mp: 4 (over z).
Axes of the slice: x: 2, y: 2, z: 4, core: 2. Of those that a mesh axis runs over, the one named last changes fastest.
Arguments:
- tokens: bfloat16 [16384, 1024], P(('dp', 'mp')), may hold values from -6 to 6
- norm_gain: float32 [2, 1024], replicated, may hold values from 0.1 to 1.9
- qkv_weight: bfloat16 [3, 1024, 1024], P(None, 'dp', 'mp')
- out_weight: bfloat16 [1024, 1024], P('mp', 'dp'), may hold values from -0.1875 to 0.1875
- variate_bias: float32 [2, 16], replicated, may hold values from -6 to 6
- ffn_weight: bfloat16 [2, 1024, 2816], P(None, 'dp', 'mp'), may hold values from -0.1875 to 0.1875
- down_weight: bfloat16 [2816, 1024], P('mp', 'dp'), may hold values from -0.109375 to 0.109375
- sample_ids: int32 [16384], P(('dp', 'mp')), may hold values from 0 to 127, as said below
- variate_ids: int32 [16384], P(('dp', 'mp')), may hold values from 0 to 15, as said below
- time_ids: int32 [16384], P(('dp', 'mp')), may hold values from 0 to 31, as said below
Outputs:
- encoded: bfloat16 [16384, 1024], P(('dp', 'mp'))
The draws below stay inside these ranges and needn't reach their ends.
Inputs may be any that keep to these rules, and one draw needn't show every extreme that they name: `sample_ids`: within each packed sequence of 512 tokens the series numbers start at 0 and never fall; a series with v variates (1 to 16) and p patches (4 to 32) holds v * p consecutive tokens, the last series of a sequence may be cut short; some packed sequence holds 128 series of one variate and four patches each. `variate_ids`: A token's offset within its series divided by that series' patch count p. `time_ids`: A token's offset within its series modulo that series' patch count p.
All inputs are finite; a program needn't handle non-finite values.
Results may differ from the reference program's by a relative error of at most 0.017.
Values may be sent and summed in bfloat16 or wider, within the bound.
A program may use at most 128 MiB of HBM per device.

```python
import jax
import jax.numpy as jnp
from jax import lax

D = 1024
HEAD_DIM = 64
HEADS = 16
FF = 2816
L = 512
SEQS = 32
TOKENS = 16384


def packing(key):
    key_var, key_pat, key_pick = jax.random.split(jax.random.fold_in(key, 5), 3)
    slots = L // 4
    variates = jax.random.randint(key_var, (SEQS, slots), 1, 17)
    patches = jax.random.randint(key_pat, (SEQS, slots), 4, 33)
    chosen = jax.random.randint(key_pick, (), 0, SEQS)
    dense = (jnp.arange(SEQS, dtype=jnp.int32) == chosen)[:, None]
    variates = jnp.where(dense, 1, variates)
    patches = jnp.where(dense, 4, patches)
    lengths = variates * patches
    ends = jnp.cumsum(lengths, axis=1)
    starts = ends - lengths
    position = jnp.arange(L, dtype=jnp.int32)
    series = jnp.sum((position[None, :, None] >= ends[:, None, :]).astype(jnp.int32), axis=2)
    begin = jnp.take_along_axis(starts, series, axis=1)
    span = jnp.take_along_axis(patches, series, axis=1)
    offset = position[None, :] - begin
    return (series.reshape(-1).astype(jnp.int32), (offset // span).reshape(-1).astype(jnp.int32), (offset % span).reshape(-1).astype(jnp.int32))


def draw_sample_ids(key, part):
    return packing(key)[0]


def draw_variate_ids(key, part):
    return packing(key)[1]


def draw_time_ids(key, part):
    return packing(key)[2]


def draw_qkv_weight(key, part):
    key_base = jax.random.fold_in(jax.random.fold_in(key, 11), 0)
    base = jax.random.normal(key_base, (3, D, D), jnp.float32) * D ** (-0.5)
    return base.astype(jnp.bfloat16)


def shard_levels(stream_key, extent, shards, least, top_value):
    level, own = 1.0, jax.random.fold_in(stream_key, 6)
    for dim, shards_of in shards:
        heights = jnp.exp(jax.random.uniform(jax.random.fold_in(own, dim), (shards_of,), jnp.float32, least / len(shards), top_value / len(shards)))
        level = level * jnp.repeat(heights, extent[dim] // shards_of).reshape([-1 if axis == dim else 1 for axis in range(len(extent))])
    return level


def gaussian(stream_key, dims, spread, most, pieces=(), held_as=jnp.bfloat16):
    level = shard_levels(stream_key, dims, pieces, -0.22, 0.18) if pieces else 1.0
    entries = jax.random.normal(stream_key, dims, jnp.float32) * spread * level
    return jnp.minimum(jnp.maximum(entries, -most), most).astype(held_as)


def setup_inputs(seed: int = 0) -> dict:
    keys = jax.random.split(jax.random.key(seed), 11)
    tokens = gaussian(keys[0], (TOKENS, D), 1.0, 6.0, ((0, 32),))
    norm_gain = jnp.clip(1.0 + 0.18 * jax.random.normal(keys[1], (2, D), jnp.float32), 0.1, 1.9)
    qkv_weight = draw_qkv_weight(jax.random.fold_in(keys[10], 71), 0)
    out_weight = gaussian(keys[3], (D, D), D ** -0.5, 0.1875, ((0, 4), (1, 8)))
    variate_bias = gaussian(keys[4], (2, HEADS), 1.5, 6.0, (), jnp.float32)
    ffn_weight = gaussian(keys[5], (2, D, FF), D ** -0.5, 0.1875, ((1, 8), (2, 4)))
    down_weight = gaussian(keys[6], (FF, D), FF ** -0.5, 0.109375, ((0, 4), (1, 8)))
    sample_ids = draw_sample_ids(jax.random.fold_in(keys[10], 71), 0)
    variate_ids = draw_variate_ids(jax.random.fold_in(keys[10], 71), 0)
    time_ids = draw_time_ids(jax.random.fold_in(keys[10], 71), 0)
    return dict(tokens=tokens, norm_gain=norm_gain, qkv_weight=qkv_weight, out_weight=out_weight, variate_bias=variate_bias, ffn_weight=ffn_weight, down_weight=down_weight, sample_ids=sample_ids, variate_ids=variate_ids, time_ids=time_ids)


def rms_norm(values, gain):
    wide = values.astype(jnp.float32)
    square = lax.optimization_barrier(jnp.mean(wide * wide, axis=-1, keepdims=True))
    return (wide * lax.rsqrt(square + 1e-05) * gain[None, :]).astype(jnp.bfloat16)

def rotate(values, times):
    half = values.shape[-1] // 2
    freq = 10000.0 ** (-jnp.arange(half, dtype=jnp.float32) / half)
    angle = times.astype(jnp.float32)[:, None] * freq[None, :]
    cosine = jnp.cos(angle)[:, None, :]
    sine = jnp.sin(angle)[:, None, :]
    first = values[..., :half]
    second = values[..., half:]
    return jnp.concatenate([first * cosine - second * sine, first * sine + second * cosine], axis=-1)

def reference(tokens, norm_gain, qkv_weight, out_weight, variate_bias, ffn_weight, down_weight, sample_ids, variate_ids, time_ids):
    total = tokens.shape[0]
    first_normed = rms_norm(tokens, norm_gain[0])
    query_raw = jnp.dot(first_normed, qkv_weight[0], preferred_element_type=jnp.float32)
    key_raw = jnp.dot(first_normed, qkv_weight[1], preferred_element_type=jnp.float32)
    value_raw = jnp.dot(first_normed, qkv_weight[2], preferred_element_type=jnp.float32)
    queries = rotate(query_raw.reshape(total, HEADS, HEAD_DIM), time_ids).astype(jnp.bfloat16)
    keys_rot = rotate(key_raw.reshape(total, HEADS, HEAD_DIM), time_ids).astype(jnp.bfloat16)
    values = value_raw.reshape(total, HEADS, HEAD_DIM).astype(jnp.bfloat16)
    count = total // L

    def one_sequence(args):
        qs, ks, vs, samples, variates = args
        scores = jnp.einsum('qhd,khd->hqk', qs.astype(jnp.float32), ks.astype(jnp.float32)) * HEAD_DIM ** (-0.5)
        same = variates[:, None] == variates[None, :]
        scores = scores + jnp.where(same[None], variate_bias[0][:, None, None], variate_bias[1][:, None, None])
        scores = jnp.where((samples[:, None] == samples[None, :])[None], scores, -1e+30)
        top = lax.optimization_barrier(jnp.max(scores, axis=2, keepdims=True))
        expo = jnp.exp(scores - top)
        weights = (expo / lax.optimization_barrier(jnp.sum(expo, axis=2, keepdims=True))).astype(jnp.bfloat16)
        return jnp.einsum('hqk,khd->qhd', weights.astype(jnp.float32), vs.astype(jnp.float32)).astype(jnp.bfloat16)
    attended = lax.map(one_sequence, (queries.reshape(count, L, HEADS, HEAD_DIM), keys_rot.reshape(count, L, HEADS, HEAD_DIM), values.reshape(count, L, HEADS, HEAD_DIM), sample_ids.reshape(count, L), variate_ids.reshape(count, L)))
    attended = attended.reshape(total, D)
    residual = (tokens.astype(jnp.float32) + jnp.dot(attended, out_weight, preferred_element_type=jnp.float32)).astype(jnp.bfloat16)
    second_normed = rms_norm(residual, norm_gain[1])
    gate = jnp.dot(second_normed, ffn_weight[0], preferred_element_type=jnp.float32)
    up = jnp.dot(second_normed, ffn_weight[1], preferred_element_type=jnp.float32)
    hidden = (jax.nn.silu(gate) * up).astype(jnp.bfloat16)
    return (residual.astype(jnp.float32) + jnp.dot(hidden, down_weight, preferred_element_type=jnp.float32)).astype(jnp.bfloat16)
```

```python
import functools
import math

import jax
import jax.numpy as jnp
from jax import lax
from jax.experimental import pallas as pl
from jax.experimental.pallas import tpu as pltpu
from jax.sharding import PartitionSpec as P

HEAD_DIM = 64
L = 512


def rms_norm(values, gain):
    wide = values.astype(jnp.float32)
    square = jnp.mean(wide * wide, axis=-1, keepdims=True)
    return (wide * lax.rsqrt(square + 1e-05) * gain[None, :]).astype(jnp.bfloat16)


def rotate(values, times):
    half = values.shape[-1] // 2
    freq = 10000.0 ** (-jnp.arange(half, dtype=jnp.float32) / half)
    angle = times.astype(jnp.float32)[:, None] * freq[None, :]
    cosine = jnp.cos(angle)[:, None, :]
    sine = jnp.sin(angle)[:, None, :]
    first = values[..., :half]
    second = values[..., half:]
    return jnp.concatenate(
        [first * cosine - second * sine, first * sine + second * cosine], axis=-1
    )


def rotated(raw, times):
    row_total, local_width = raw.shape
    turned = rotate(raw.reshape(row_total, local_width // HEAD_DIM, HEAD_DIM), times)
    return turned.reshape(row_total, local_width).astype(jnp.bfloat16)


def attend(queries, keys_rot, values, samples, variates, bias):
    row_total, local_width = queries.shape
    heads_here = local_width // HEAD_DIM
    count = row_total // L

    def one_sequence(args):
        qs, ks, vs, sample_row, variate_row = args
        scores = jnp.einsum(
            "qhd,khd->hqk", qs, ks, preferred_element_type=jnp.float32
        ) * HEAD_DIM ** (-0.5)
        same = variate_row[:, None] == variate_row[None, :]
        scores = scores + jnp.where(same[None], bias[0][:, None, None], bias[1][:, None, None])
        scores = jnp.where((sample_row[:, None] == sample_row[None, :])[None], scores, -1e30)
        top = jnp.max(scores, axis=2, keepdims=True)
        expo = jnp.exp(scores - top)
        weights = (expo / jnp.sum(expo, axis=2, keepdims=True)).astype(jnp.bfloat16)
        return jnp.einsum("hqk,khd->qhd", weights, vs, preferred_element_type=jnp.float32).astype(
            jnp.bfloat16
        )

    shape = (count, L, heads_here, HEAD_DIM)
    result = lax.map(
        one_sequence,
        (
            queries.reshape(shape),
            keys_rot.reshape(shape),
            values.reshape(shape),
            samples.reshape(count, L),
            variates.reshape(count, L),
        ),
    )
    return result.reshape(row_total, local_width)


def local(
    tokens,
    norm_gain,
    qkv_weight,
    out_weight,
    variate_bias,
    ffn_weight,
    down_weight,
    sample_ids,
    variate_ids,
    time_ids,
):
    first_normed = rms_norm(tokens, norm_gain[0])
    wide_columns = lax.all_gather(qkv_weight, "mp", axis=2, tiled=True)
    columns = first_normed
    projected = jnp.einsum(
        "rc,jcd->jrd",
        columns,
        lax.all_gather(wide_columns, "dp", axis=1, tiled=True),
        preferred_element_type=jnp.float32,
    )
    queries = rotated(projected[0], time_ids)
    keys_rot = rotated(projected[1], time_ids)
    values = projected[2].astype(jnp.bfloat16)
    back_rows = attend(queries, keys_rot, values, sample_ids, variate_ids, variate_bias)
    out_rows = lax.all_gather(out_weight, "mp", axis=0, tiled=True)
    mixed = jnp.dot(
        back_rows,
        lax.all_gather(out_rows, "dp", axis=1, tiled=True),
        preferred_element_type=jnp.float32,
    )
    residual = (tokens.astype(jnp.float32) + mixed).astype(jnp.bfloat16)
    second_normed = rms_norm(residual, norm_gain[1])
    ffn_columns = lax.all_gather(ffn_weight, "mp", axis=2, tiled=True)
    columns = second_normed
    gate_up = jnp.einsum(
        "rc,jcf->jrf",
        columns,
        lax.all_gather(ffn_columns, "dp", axis=1, tiled=True),
        preferred_element_type=jnp.float32,
    )
    hidden = (jax.nn.silu(gate_up[0]) * gate_up[1]).astype(jnp.bfloat16)
    down_full = lax.all_gather(down_weight, "mp", axis=0, tiled=True)
    feed = jnp.dot(
        hidden,
        lax.all_gather(down_full, "dp", axis=1, tiled=True),
        preferred_element_type=jnp.float32,
    )
    return (residual.astype(jnp.float32) + feed).astype(jnp.bfloat16)

MESH = pl.DeviceIdType.MESH
WIDE = 2 * HEAD_DIM
ROWS = 256
LAYOUT = (2 ** 3, 2 ** 2)
HALVES = 2
FF_PARTS = 4
LOG2E = math.log2(math.e)
SLOTS = ("zp", "zoE", "zoM", "zf", "p1", "p2", "a1", "a2")
KINDS = "AAAAAAABBAAAAAAABBAA"
LEADS = "xyxyxyxxyyxyxyxyxyxy"
PLAN = (
    ((0, 0), (1, 0), (16, 0), (7, 0), (8, 0), (4, 0), (3, 0), (2, 0),),
    (),
    (),
    ((0, 1), (16, 1), (1, 1), (7, 1), (8, 1), (17, 0), (0, 2), (1, 2), (4, 1), (3, 1), (2, 1), (5, 0), (6, 0), (4, 2), (10, 0), (3, 2), (2, 2), (17, 1), (11, 0), (9, 0), (13, 0), (0, 3), (1, 3), (5, 1), (12, 0), (14, 0), (6, 1), (10, 1), (4, 3), (3, 3), (15, 0), (5, 2), (2, 3), (6, 2), (11, 1), (9, 1), (10, 2), (13, 1), (18, 0), (19, 0), (0, 4), (11, 2), (12, 1), (14, 1), (1, 4), (9, 2), (0, 5),),
    (),
    ((13, 2), (1, 5), (16, 2), (15, 1), (7, 2),),
    (),
    ((12, 2), (14, 2), (4, 4), (3, 4), (5, 3), (8, 2), (2, 4), (6, 3), (4, 5), (3, 5), (18, 1), (19, 1), (2, 5), (10, 3),),
    (),
    (),
    ((15, 2),),
    ((11, 3),),
    (),
    (),
    (),
    (),
    (),
    (),
    (),
    (),
    (),
    ((18, 2), (16, 3), (19, 2), (9, 3), (7, 3), (13, 3), (8, 3), (17, 2), (12, 3), (14, 3), (5, 4), (6, 4), (5, 5),),
    (),
    (),
    (),
    (),
    (),
    (),
    ((15, 3), (10, 4), (6, 5), (16, 4),),
    (),
    ((7, 4),),
    ((10, 5), (16, 5), (7, 5), (18, 3), (19, 3), (11, 4),),
    (),
    (),
    (),
    (),
    ((8, 4), (9, 4), (13, 4), (17, 3), (11, 5), (8, 5),),
    ((9, 5),),
    ((13, 5), (12, 4),),
    (),
    (),
    ((14, 4), (12, 5),),
    (),
    ((14, 5), (15, 4),),
    (),
    ((15, 5), (17, 4),),
    (),
    (),
    ((18, 4), (17, 5),),
    ((19, 4), (18, 5),),
    ((19, 5),),
    (),
)


def stages(kind, lead):
    other = "y" if lead == "x" else "x"
    if kind == "A":
        return [
            ((), (("zp", "z"), ("zo", "z"))),
            (("ZM",), (("zf", "z"),)),
            (("ZP", "ZF"), (("p1", lead),)),
            (("p1",), (("p2", other), ("a1", "c"))),
            (("p2",), (("a2", "c"),)),
            (("a1", "a2"), ()),
        ]
    return [
        ((), (("p1", lead),)),
        (("p1",), (("p2", other),)),
        (("p2",), (("zp", "z"), ("zo", "z"))),
        (("ZM",), (("zf", "z"),)),
        (("ZP", "ZF"), (("a2", "c"),)),
        (("a2",), ()),
    ]


def layer_kernel(
    spans,
    bias_ref, gain_ref, sample_ref, variate_ref, time_ref, tokens_in, qkv_in, out_in, ffn_in, down_in,
    final_ref,
    weights, tokens, normed, queries, keys, values, attended, residual, gate, hidden, total,
    cosine, sine, kinds, mask, result, send_sem, recv_sem, local_sem, token_sem, result_sem,
):
    dp = lax.axis_index("dp")
    z = lax.axis_index("mp")
    core = lax.rem(dp, 2)
    x = lax.rem(dp // 2, 2)
    y = dp // 4
    whole = slice(None)
    is_mid = jnp.logical_or(z == 1, z == 2)
    low = z < 2
    partner_z = z + 1 - 2 * lax.rem(z, 2)
    far_mid = jnp.where(low, 2, 1)
    far_end = jnp.where(low, 3, 0)
    far_half = pl.ds(jnp.where(low, 2, 0), 2)
    to = {
        "x": {"dp": (y * 2 + 1 - x) * 2 + core, "mp": z},
        "y": {"dp": ((1 - y) * 2 + x) * 2 + core, "mp": z},
        "c": {"dp": (y * 2 + x) * 2 + 1 - core, "mp": z},
        "zp": {"dp": dp, "mp": partner_z},
        "zo": {"dp": dp, "mp": far_mid},
        "far": {"dp": dp, "mp": far_end},
    }
    to["zf"] = to["zp"]

    def region(chunk, name):
        kind, lead = KINDS[chunk], LEADS[chunk]
        if name in ("zp", "zo"):
            head = (y, x, core, z) if kind == "A" else (whole, whole, core, z)
        elif name == "zf":
            head = (y, x, core, far_half) if kind == "A" else (whole, whole, core, far_half)
        elif name == "p1":
            head = (y, x, core, whole) if kind == "A" else (y, x, core, z)
        else:
            cut = slice(None) if kind == "A" else z
            if name == "p2":
                head = ((y, whole) if lead == "x" else (whole, x)) + (core, cut)
            elif name == "a1":
                head = ((y, whole) if lead == "x" else (whole, x)) + (core, whole)
            elif kind == "A":
                head = ((1 - y, whole) if lead == "x" else (whole, 1 - x)) + (core, whole)
            else:
                head = (whole, whole, core, whole)
        start, rows = spans[chunk]
        return head + (pl.ds(start, rows),)

    def copy(chunk, name, target, landing=None):
        part = weights.at[region(chunk, name)]
        slot = chunk * len(SLOTS)
        if name == "zo" and landing is None:
            slot = slot + jnp.where(is_mid, SLOTS.index("zoM"), SLOTS.index("zoE"))
        else:
            slot = slot + SLOTS.index(landing or name)
        return pltpu.make_async_remote_copy(
            src_ref=part, dst_ref=part, send_sem=send_sem.at[slot], recv_sem=recv_sem.at[slot],
            device_id=target, device_id_type=MESH,
        )

    def axis_of(chunk, name):
        lead = LEADS[chunk]
        other = "y" if lead == "x" else "x"
        return {"p1": lead, "p2": other, "a1": "c", "a2": "c"}.get(name, name)

    def wait_for(chunk, mark):
        if mark == "ZM":
            @pl.when(is_mid)
            def _():
                copy(chunk, "zo", to["zo"], "zoE").wait_recv()
                copy(chunk, "zo", to["zo"], "zoM").wait_recv()
        elif mark == "ZP":
            copy(chunk, "zp", to["zp"]).wait_recv()
        elif mark == "ZF":
            @pl.when(jnp.logical_not(is_mid))
            def _():
                copy(chunk, "zf", to["zf"]).wait_recv()
        else:
            copy(chunk, mark, to[axis_of(chunk, mark)]).wait_recv()

    def event(chunk, stage):
        waits, sends = stages(KINDS[chunk], LEADS[chunk])[stage]
        for mark in waits:
            wait_for(chunk, mark)
        for name, _ in sends:
            begin = copy(chunk, name, to[axis_of(chunk, name)]).start
            if name == "zf":
                pl.when(is_mid)(begin)
            else:
                begin()

    def all_sent():
        for chunk in range(len(KINDS)):
            for _, sends in stages(KINDS[chunk], LEADS[chunk]):
                for name, _ in sends:
                    finish = copy(chunk, name, to[axis_of(chunk, name)]).wait_send
                    if name == "zf":
                        pl.when(is_mid)(finish)
                    else:
                        finish()

    cursor = [0]

    def now():
        for item in PLAN[cursor[0]]:
            event(*item)
        cursor[0] += 1

    def steps(count):
        plan = PLAN[cursor[0]:cursor[0] + count]
        cursor[0] += count

        def run(step):
            for place, items in enumerate(plan):
                if items:
                    @pl.when(step == place)
                    def _():
                        for item in items:
                            event(*item)
        return run

    mine = weights.at[y, x, core, z]
    own = []
    row = 0
    for half in range(HALVES):
        for kind in range(3):
            own.append((qkv_in.at[kind, :, pl.ds(half * WIDE, WIDE)], row, qkv_in.shape[1]))
            row += qkv_in.shape[1]
    own.append((out_in, row, out_in.shape[0]))
    row += out_in.shape[0]
    part = ffn_in.shape[1] // FF_PARTS
    for index in range(FF_PARTS):
        for source in (ffn_in.at[0], ffn_in.at[1], down_in):
            own.append((source.at[pl.ds(index * part, part)], row, part))
            row += part
    loads = [
        pltpu.make_async_copy(source, mine.at[pl.ds(at, rows)], local_sem.at[place])
        for place, (source, at, rows) in enumerate(own)
    ]
    token_load = pltpu.make_async_copy(tokens_in, tokens, token_sem)
    for load in loads:
        load.start()
    token_load.start()
    barrier = pltpu.get_barrier_semaphore()
    for peer in ("x", "y", "c", "zp", "zo", "far"):
        pl.semaphore_signal(barrier, inc=1, device_id=to[peer], device_id_type=MESH)
    pl.semaphore_wait(barrier, 6)
    for load in loads:
        load.wait()
    now()

    total_rows, width = tokens.shape
    blocks = total_rows // ROWS

    def norm_rows(source, gain_row):
        gain = gain_ref[gain_row:gain_row + 1, :]

        def body(step, carry):
            rows = pl.ds(pl.multiple_of(step * 128, 128), 128)
            wide = source[rows, :].astype(jnp.float32)
            square = jnp.mean(wide * wide, axis=-1, keepdims=True)
            normed[rows, :] = (wide * lax.rsqrt(square + 1e-05) * gain).astype(jnp.bfloat16)
            return carry
        lax.fori_loop(0, total_rows // 128, body, 0)

    token_load.wait()
    now()
    norm_rows(tokens, 0)
    now()
    lane = lax.broadcasted_iota(jnp.int32, (1, WIDE), 1)
    half_head = HEAD_DIM // 2
    times = jnp.broadcast_to(time_ref[...].astype(jnp.float32), (WIDE, total_rows)).T
    freq = jnp.exp(lax.rem(lane, half_head).astype(jnp.float32) * (-math.log(10000.0) / half_head))
    front = lax.rem(lane, HEAD_DIM) < half_head
    angle = times * freq
    cosine[...] = jnp.cos(angle)
    sine[...] = jnp.where(front, -1.0, 1.0) * jnp.sin(angle)
    variates = jnp.broadcast_to(variate_ref[...].astype(jnp.float32), (WIDE, total_rows)).T
    spare = lax.rem(lane, HEAD_DIM)
    number = lax.rem(spare, 16).astype(jnp.float32)
    third = spare // 16
    kinds[...] = jnp.where(
        jnp.logical_and(variates == number, third < 3), 1.0, 0.0
    ).astype(jnp.bfloat16)
    samples = sample_ref[...].astype(jnp.float32)
    for quarter in range(total_rows // WIDE):
        rows = slice(quarter * WIDE, (quarter + 1) * WIDE)
        column = jnp.broadcast_to(samples[:, rows], (WIDE, WIDE)).T
        for piece in range(L // WIDE):
            base = quarter * WIDE // L * L + piece * WIDE
            other = samples[:, base:base + WIDE]
            mask[rows, piece * WIDE:(piece + 1) * WIDE] = jnp.where(column == other, 0.0, -1e30)

    left = lane < HEAD_DIM

    def rows_of(at, count, index):
        return jnp.concatenate(
            [
                weights[a, b, c, index, pl.ds(at, count), :]
                for a in range(2) for b in range(2) for c in range(2)
            ],
            axis=0,
        )

    def rotated(raw, factor):
        swapped = jnp.where(
            front, pltpu.roll(raw, WIDE - half_head, 1), pltpu.roll(raw, half_head, 1)
        )
        return ((raw * cosine[...] + swapped * sine[...]) * factor).astype(jnp.bfloat16)

    def project(half, at, kind, held, run, base):
        def body(step, carry):
            run(base + step)
            weight = jnp.concatenate(
                [rows_of(at, width // 8, step * 2), rows_of(at, width // 8, step * 2 + 1)], axis=1
            )
            raw = jnp.dot(normed[...], weight, preferred_element_type=jnp.float32)
            for group in range(2):
                piece = raw[:, group * WIDE:(group + 1) * WIDE]
                if kind == 0:
                    piece = rotated(piece, HEAD_DIM ** -0.5 * LOG2E)
                elif kind == 1:
                    piece = rotated(piece, 1.0)
                else:
                    piece = piece.astype(jnp.bfloat16)
                held[(step * 2 + group) * HALVES + half] = piece
            return carry
        lax.fori_loop(0, 2, body, 0)

    def attend(half, run):
        def body(step, carry):
            run(step)
            pair = step // blocks * HALVES + half
            block = lax.rem(step, blocks)
            rows = pl.ds(pl.multiple_of(block * ROWS, ROWS), ROWS)
            span = pl.ds(pl.multiple_of((block * ROWS) // L * L, L), L)
            both = queries[pair, rows, :]
            key_rows = keys[pair, span, :]
            value_rows = values[pair, span, :]
            own_kinds = kinds[rows, :]
            other_kinds = kinds[span, :]
            one = jnp.ones((), jnp.bfloat16)
            mixed = []
            for side in range(2):
                head = pair * 2 + side
                chosen = left if side == 0 else jnp.logical_not(left)
                gap = jnp.full((1, WIDE), (bias_ref[0, head] - bias_ref[1, head]) * LOG2E, jnp.float32)
                first = gap.astype(jnp.bfloat16).astype(jnp.float32)
                second = (gap - first).astype(jnp.bfloat16).astype(jnp.float32)
                parts = jnp.where(third == 0, first, jnp.where(third == 1, second, gap - first - second))
                query = jnp.where(chosen, both, own_kinds * parts.astype(jnp.bfloat16))
                key = jnp.where(chosen, key_rows, other_kinds)
                value = jnp.where(chosen, value_rows, one)
                scores = lax.dot_general(
                    query, key, (((1,), (1,)), ((), ())), preferred_element_type=jnp.float32
                )
                scores = scores + mask[rows, :]
                top = jnp.max(scores, axis=1, keepdims=True)
                expo = jnp.exp2(scores - top).astype(jnp.bfloat16)
                mixed.append(jnp.dot(expo, value, preferred_element_type=jnp.float32))
            amount = jnp.where(left, mixed[0], mixed[1])
            share = pltpu.roll(jnp.where(left, mixed[1], mixed[0]), HEAD_DIM, 1)
            lanes = pl.ds(pl.multiple_of(pair * WIDE, WIDE), WIDE)
            attended[rows, lanes] = (amount / share).astype(jnp.bfloat16)
            return carry
        lax.fori_loop(0, width // WIDE // HALVES * blocks, body, 0)

    for half in range(HALVES):
        run = steps(6)
        for kind, held in enumerate((queries, keys, values)):
            project(half, spans[half * 3 + kind][0], kind, held, run, kind * 2)
        attend(half, steps(width // WIDE // HALVES * blocks))

    def columns_of(at, count, side_y, side_x):
        return jnp.concatenate(
            [
                jnp.concatenate(
                    [weights[side_y, side_x, c, index, pl.ds(at, count), :] for c in range(2)], axis=1
                )
                for index in range(LAYOUT[1])
            ],
            axis=0,
        )

    slab = 2 * WIDE
    out_at = spans[HALVES * 3][0]
    out_events = steps(4)

    def out_step(step, carry):
        out_events(step)
        lanes = pl.ds(pl.multiple_of(step * slab, slab), slab)
        weight = columns_of(out_at, width // LAYOUT[1], step // 2, lax.rem(step, 2))
        mixed = jnp.dot(attended[...], weight, preferred_element_type=jnp.float32)
        wide = (tokens[:, lanes].astype(jnp.float32) + mixed).astype(jnp.bfloat16)
        residual[:, lanes] = wide
        total[:, lanes] = wide.astype(jnp.float32)
        return carry
    lax.fori_loop(0, 4, out_step, 0)
    now()
    norm_rows(residual, 1)

    def hidden_weight(at):
        return jnp.concatenate(
            [
                jnp.concatenate(
                    [
                        weights[a, b, c, index, pl.ds(at, part), :]
                        for a in range(2) for b in range(2) for c in range(2)
                    ],
                    axis=1,
                )
                for index in range(LAYOUT[1])
            ],
            axis=0,
        )

    def against(at):
        return lax.dot_general(
            normed[...], hidden_weight(at), (((1,), (1,)), ((), ())),
            preferred_element_type=jnp.float32,
        )

    ff_at = spans[HALVES * 3 + 2][0]
    ff_events = steps(FF_PARTS * 4)

    def ff_step(index, carry):
        at = ff_at + index * (3 * part)
        at = pl.multiple_of(at, 16)
        ff_events(index * 4)
        gate[...] = against(at)
        ff_events(index * 4 + 1)
        up = against(pl.multiple_of(at + part, 16))
        opened = gate[...]
        hidden[...] = (opened / (1.0 + jnp.exp(-opened)) * up).astype(jnp.bfloat16)
        for pair in range(2):
            ff_events(index * 4 + 2 + pair)
            for side in range(2):
                lanes = slice((pair * 2 + side) * slab, (pair * 2 + side + 1) * slab)
                weight = columns_of(pl.multiple_of(at + 2 * part, 16), part, pair, side)
                fresh = total[:, lanes] + jnp.dot(
                    hidden[...], weight, preferred_element_type=jnp.float32
                )
                total[:, lanes] = fresh
        return carry
    lax.fori_loop(0, FF_PARTS, ff_step, 0)
    for piece in range(4):
        lanes = slice(piece * slab, (piece + 1) * slab)
        result[:, lanes] = total[:, lanes].astype(jnp.bfloat16)
    save = pltpu.make_async_copy(result, final_ref, result_sem)
    save.start()
    all_sent()
    save.wait()


def spans_of(qkv, out, ffn):
    found, row = [], 0
    for rows in [qkv.shape[1]] * (3 * HALVES) + [out.shape[0] // 2] * 2 + [ffn.shape[1] // FF_PARTS] * (3 * FF_PARTS):
        found.append((row, rows))
        row += rows
    return tuple(found), row


def fused(
    tokens, norm_gain, qkv_weight, out_weight, variate_bias, ffn_weight, down_weight,
    sample_ids, variate_ids, time_ids,
):
    rows, width = tokens.shape
    ffn = jnp.swapaxes(ffn_weight, 1, 2)
    spans, depth = spans_of(qkv_weight, out_weight, ffn)
    vmem = pl.BlockSpec(memory_space=pltpu.VMEM)
    anywhere = pl.BlockSpec(memory_space=pl.ANY)
    per_pair = pltpu.VMEM((width // WIDE, rows, WIDE), jnp.bfloat16)
    flat = pltpu.VMEM((rows, width), jnp.bfloat16)
    strip = pltpu.VMEM((rows, WIDE), jnp.float32)
    ff_wide = LAYOUT[1] * ffn.shape[1] // FF_PARTS
    copies = len(KINDS) * len(SLOTS)
    return pl.pallas_call(
        functools.partial(layer_kernel, spans),
        out_shape=jax.ShapeDtypeStruct((rows, width), jnp.bfloat16),
        in_specs=[pl.BlockSpec(memory_space=pltpu.SMEM)] + [vmem] * 4 + [anywhere] * 5,
        out_specs=anywhere,
        scratch_shapes=[
            pltpu.VMEM((2, 2, 2, LAYOUT[1], depth, WIDE), jnp.bfloat16),
            flat, flat, per_pair, per_pair, per_pair, flat, flat,
            pltpu.VMEM((rows, ff_wide), jnp.float32),
            pltpu.VMEM((rows, ff_wide), jnp.bfloat16),
            pltpu.VMEM((rows, width), jnp.float32),
            strip, strip, pltpu.VMEM((rows, WIDE), jnp.bfloat16),
            pltpu.VMEM((rows, L), jnp.float32),
            flat,
            pltpu.SemaphoreType.DMA((copies,)),
            pltpu.SemaphoreType.DMA((copies,)),
            pltpu.SemaphoreType.DMA((3 * HALVES + 1 + 3 * FF_PARTS,)),
            pltpu.SemaphoreType.DMA(()),
            pltpu.SemaphoreType.DMA(()),
        ],
        compiler_params=pltpu.CompilerParams(
            collective_id=0, has_side_effects=True, vmem_limit_bytes=60 * 1024 * 1024
        ),
    )(
        variate_bias, norm_gain, sample_ids.reshape(1, -1), variate_ids.reshape(1, -1),
        time_ids.reshape(1, -1), tokens, qkv_weight, out_weight, ffn, down_weight,
    )


def solution(mesh):
    body = fused if (mesh.shape["dp"], mesh.shape["mp"]) == LAYOUT else local
    return jax.shard_map(
        body,
        mesh=mesh,
        in_specs=(
            P(("dp", "mp"), None),
            P(),
            P(None, "dp", "mp"),
            P("mp", "dp"),
            P(),
            P(None, "dp", "mp"),
            P("mp", "dp"),
            P(("dp", "mp")),
            P(("dp", "mp")),
            P(("dp", "mp")),
        ),
        out_specs=P(("dp", "mp"), None),
        check_vma=False,
    )
```

```python
import functools
import math

import jax
import jax.numpy as jnp
from jax import lax
from jax.experimental import pallas as pl
from jax.experimental.pallas import tpu as pltpu
from jax.sharding import PartitionSpec as P

HEAD_DIM = 64
L = 512


def rms_norm(values, gain):
    wide = values.astype(jnp.float32)
    square = jnp.mean(wide * wide, axis=-1, keepdims=True)
    return (wide * lax.rsqrt(square + 1e-05) * gain[None, :]).astype(jnp.bfloat16)


def rotate(values, times):
    half = values.shape[-1] // 2
    freq = 10000.0 ** (-jnp.arange(half, dtype=jnp.float32) / half)
    angle = times.astype(jnp.float32)[:, None] * freq[None, :]
    cosine = jnp.cos(angle)[:, None, :]
    sine = jnp.sin(angle)[:, None, :]
    first = values[..., :half]
    second = values[..., half:]
    return jnp.concatenate(
        [first * cosine - second * sine, first * sine + second * cosine], axis=-1
    )


def rotated(raw, times):
    row_total, local_width = raw.shape
    turned = rotate(raw.reshape(row_total, local_width // HEAD_DIM, HEAD_DIM), times)
    return turned.reshape(row_total, local_width).astype(jnp.bfloat16)


def attend(queries, keys_rot, values, samples, variates, bias):
    row_total, local_width = queries.shape
    heads_here = local_width // HEAD_DIM
    count = row_total // L

    def one_sequence(args):
        qs, ks, vs, sample_row, variate_row = args
        scores = jnp.einsum(
            "qhd,khd->hqk", qs, ks, preferred_element_type=jnp.float32
        ) * HEAD_DIM ** (-0.5)
        same = variate_row[:, None] == variate_row[None, :]
        scores = scores + jnp.where(same[None], bias[0][:, None, None], bias[1][:, None, None])
        scores = jnp.where((sample_row[:, None] == sample_row[None, :])[None], scores, -1e30)
        top = jnp.max(scores, axis=2, keepdims=True)
        expo = jnp.exp(scores - top)
        weights = (expo / jnp.sum(expo, axis=2, keepdims=True)).astype(jnp.bfloat16)
        return jnp.einsum("hqk,khd->qhd", weights, vs, preferred_element_type=jnp.float32).astype(
            jnp.bfloat16
        )

    shape = (count, L, heads_here, HEAD_DIM)
    result = lax.map(
        one_sequence,
        (
            queries.reshape(shape),
            keys_rot.reshape(shape),
            values.reshape(shape),
            samples.reshape(count, L),
            variates.reshape(count, L),
        ),
    )
    return result.reshape(row_total, local_width)


def local(
    tokens,
    norm_gain,
    qkv_weight,
    out_weight,
    variate_bias,
    ffn_weight,
    down_weight,
    sample_ids,
    variate_ids,
    time_ids,
):
    first_normed = rms_norm(tokens, norm_gain[0])
    wide_columns = lax.all_gather(qkv_weight, "mp", axis=2, tiled=True)
    columns = first_normed
    projected = jnp.einsum(
        "rc,jcd->jrd",
        columns,
        lax.all_gather(wide_columns, "dp", axis=1, tiled=True),
        preferred_element_type=jnp.float32,
    )
    queries = rotated(projected[0], time_ids)
    keys_rot = rotated(projected[1], time_ids)
    values = projected[2].astype(jnp.bfloat16)
    back_rows = attend(queries, keys_rot, values, sample_ids, variate_ids, variate_bias)
    out_rows = lax.all_gather(out_weight, "mp", axis=0, tiled=True)
    mixed = jnp.dot(
        back_rows,
        lax.all_gather(out_rows, "dp", axis=1, tiled=True),
        preferred_element_type=jnp.float32,
    )
    residual = (tokens.astype(jnp.float32) + mixed).astype(jnp.bfloat16)
    second_normed = rms_norm(residual, norm_gain[1])
    ffn_columns = lax.all_gather(ffn_weight, "mp", axis=2, tiled=True)
    columns = second_normed
    gate_up = jnp.einsum(
        "rc,jcf->jrf",
        columns,
        lax.all_gather(ffn_columns, "dp", axis=1, tiled=True),
        preferred_element_type=jnp.float32,
    )
    hidden = (jax.nn.silu(gate_up[0]) * gate_up[1]).astype(jnp.bfloat16)
    down_full = lax.all_gather(down_weight, "mp", axis=0, tiled=True)
    feed = jnp.dot(
        hidden,
        lax.all_gather(down_full, "dp", axis=1, tiled=True),
        preferred_element_type=jnp.float32,
    )
    return (residual.astype(jnp.float32) + feed).astype(jnp.bfloat16)

MESH = pl.DeviceIdType.MESH
WIDE = 2 * HEAD_DIM
ROWS = 512
LAYOUT = (2 ** 3, 2 ** 2)
HALVES = 2
FF_PARTS = 4
LOG2E = math.log2(math.e)
SLOTS = ("zp", "zoE", "zoM", "zf", "p1", "p2", "a1", "a2")
KINDS = "AAAAAAAAAAABABABABAA"
LEADS = "xyxyxxyyyxxxyyxxyyxy"
PLAN = (
    ((1, 0), (13, 0), (0, 0), (11, 0), (3, 0), (2, 0), (7, 0), (17, 0), (5, 0), (15, 0),),
    (),
    (),
    ((1, 1), (11, 1), (15, 1), (17, 1), (0, 1), (13, 1), (3, 1), (1, 2), (2, 1), (0, 2), (7, 1), (6, 0), (3, 2), (9, 0), (5, 1), (10, 0), (4, 0), (2, 2), (7, 2), (12, 0), (8, 0), (6, 1), (16, 0), (1, 3), (0, 3), (5, 2), (4, 1), (12, 1), (6, 2), (19, 0), (3, 3), (4, 2), (18, 0), (14, 0), (8, 1), (2, 3), (8, 2), (10, 1), (9, 1), (0, 4), (3, 4), (16, 1), (7, 3), (14, 1), (12, 2), (13, 2), (6, 3), (18, 1), (5, 3), (9, 2), (14, 2), (16, 2), (11, 2), (15, 2), (10, 2), (19, 1), (4, 3), (8, 3), (7, 4), (6, 4), (2, 4), (1, 4), (2, 5), (1, 5), (6, 5), (18, 2), (0, 5),),
    ((9, 3), (13, 3), (5, 4),),
    (),
    (),
    (),
    (),
    (),
    ((19, 2),),
    (),
    ((4, 4), (12, 3), (10, 3), (11, 3),),
    ((13, 4), (15, 3), (14, 3), (5, 5), (17, 2), (3, 5),),
    (),
    ((13, 5), (4, 5),),
    (),
    (),
    (),
    ((8, 4), (7, 5), (16, 3), (9, 4),),
    (),
    (),
    ((18, 3), (8, 5),),
    (),
    (),
    (),
    (),
    (),
    (),
    ((10, 4), (12, 4), (11, 4), (19, 3), (10, 5), (9, 5), (17, 3),),
    (),
    (),
    ((11, 5), (15, 4),),
    ((14, 4), (16, 4), (12, 5),),
    (),
    ((14, 5), (15, 5),),
    (),
    (),
    ((17, 4), (16, 5),),
    (),
    ((18, 4), (19, 4), (17, 5),),
    ((18, 5),),
    ((19, 5),),
    (),
)


def stages(kind, lead):
    other = "y" if lead == "x" else "x"
    if kind == "A":
        return [
            ((), (("zp", "z"), ("zo", "z"))),
            (("ZM",), (("zf", "z"),)),
            (("ZP", "ZF"), (("p1", lead),)),
            (("p1",), (("p2", other), ("a1", "c"))),
            (("p2",), (("a2", "c"),)),
            (("a1", "a2"), ()),
        ]
    return [
        ((), (("p1", lead),)),
        (("p1",), (("p2", other),)),
        (("p2",), (("zp", "z"), ("zo", "z"))),
        (("ZM",), (("zf", "z"),)),
        (("ZP", "ZF"), (("a2", "c"),)),
        (("a2",), ()),
    ]


def layer_kernel(
    spans,
    bias_ref, gain_ref, sample_ref, variate_ref, time_ref, tokens_in, qkv_in, out_in, ffn_in, down_in,
    final_ref,
    weights, tokens, normed, queries, keys, values, attended, residual, gate, hidden, total,
    cosine, sine, kinds, mask, send_sem, recv_sem, local_sem, token_sem,
):
    dp = lax.axis_index("dp")
    z = lax.axis_index("mp")
    core = lax.rem(dp, 2)
    x = lax.rem(dp // 2, 2)
    y = dp // 4
    whole = slice(None)
    is_mid = jnp.logical_or(z == 1, z == 2)
    low = z < 2
    partner_z = z + 1 - 2 * lax.rem(z, 2)
    far_mid = jnp.where(low, 2, 1)
    far_end = jnp.where(low, 3, 0)
    far_half = pl.ds(jnp.where(low, 2, 0), 2)
    to = {
        "x": {"dp": (y * 2 + 1 - x) * 2 + core, "mp": z},
        "y": {"dp": ((1 - y) * 2 + x) * 2 + core, "mp": z},
        "c": {"dp": (y * 2 + x) * 2 + 1 - core, "mp": z},
        "zp": {"dp": dp, "mp": partner_z},
        "zo": {"dp": dp, "mp": far_mid},
        "far": {"dp": dp, "mp": far_end},
    }
    to["zf"] = to["zp"]

    def region(chunk, name):
        kind, lead = KINDS[chunk], LEADS[chunk]
        if name in ("zp", "zo"):
            head = (y, x, core, z) if kind == "A" else (whole, whole, core, z)
        elif name == "zf":
            head = (y, x, core, far_half) if kind == "A" else (whole, whole, core, far_half)
        elif name == "p1":
            head = (y, x, core, whole) if kind == "A" else (y, x, core, z)
        else:
            cut = slice(None) if kind == "A" else z
            if name == "p2":
                head = ((y, whole) if lead == "x" else (whole, x)) + (core, cut)
            elif name == "a1":
                head = ((y, whole) if lead == "x" else (whole, x)) + (core, whole)
            elif kind == "A":
                head = ((1 - y, whole) if lead == "x" else (whole, 1 - x)) + (core, whole)
            else:
                head = (whole, whole, core, whole)
        start, rows = spans[chunk]
        return head + (pl.ds(start, rows),)

    def copy(chunk, name, target, landing=None):
        part = weights.at[region(chunk, name)]
        slot = chunk * len(SLOTS)
        if name == "zo" and landing is None:
            slot = slot + jnp.where(is_mid, SLOTS.index("zoM"), SLOTS.index("zoE"))
        else:
            slot = slot + SLOTS.index(landing or name)
        return pltpu.make_async_remote_copy(
            src_ref=part, dst_ref=part, send_sem=send_sem.at[slot], recv_sem=recv_sem.at[slot],
            device_id=target, device_id_type=MESH,
        )

    def axis_of(chunk, name):
        lead = LEADS[chunk]
        other = "y" if lead == "x" else "x"
        return {"p1": lead, "p2": other, "a1": "c", "a2": "c"}.get(name, name)

    def wait_for(chunk, mark):
        if mark == "ZM":
            @pl.when(is_mid)
            def _():
                copy(chunk, "zo", to["zo"], "zoE").wait_recv()
                copy(chunk, "zo", to["zo"], "zoM").wait_recv()
        elif mark == "ZP":
            copy(chunk, "zp", to["zp"]).wait_recv()
        elif mark == "ZF":
            @pl.when(jnp.logical_not(is_mid))
            def _():
                copy(chunk, "zf", to["zf"]).wait_recv()
        else:
            copy(chunk, mark, to[axis_of(chunk, mark)]).wait_recv()

    def event(chunk, stage):
        waits, sends = stages(KINDS[chunk], LEADS[chunk])[stage]
        for mark in waits:
            wait_for(chunk, mark)
        for name, _ in sends:
            begin = copy(chunk, name, to[axis_of(chunk, name)]).start
            if name == "zf":
                pl.when(is_mid)(begin)
            else:
                begin()

    def all_sent():
        for chunk in range(len(KINDS)):
            for _, sends in stages(KINDS[chunk], LEADS[chunk]):
                for name, _ in sends:
                    finish = copy(chunk, name, to[axis_of(chunk, name)]).wait_send
                    if name == "zf":
                        pl.when(is_mid)(finish)
                    else:
                        finish()

    cursor = [0]

    def now():
        for item in PLAN[cursor[0]]:
            event(*item)
        cursor[0] += 1

    def steps(count):
        plan = PLAN[cursor[0]:cursor[0] + count]
        cursor[0] += count

        def run(step):
            for place, items in enumerate(plan):
                if items:
                    @pl.when(step == place)
                    def _():
                        for item in items:
                            event(*item)
        return run

    mine = weights.at[y, x, core, z]
    own = []
    row = 0
    for half in range(HALVES):
        for kind in range(3):
            own.append((qkv_in.at[kind, :, pl.ds(half * WIDE, WIDE)], row, qkv_in.shape[1]))
            row += qkv_in.shape[1]
    own.append((out_in, row, out_in.shape[0]))
    row += out_in.shape[0]
    part = ffn_in.shape[1] // FF_PARTS
    for index in range(FF_PARTS):
        for source in (ffn_in.at[0], ffn_in.at[1], down_in):
            own.append((source.at[pl.ds(index * part, part)], row, part))
            row += part
    loads = [
        pltpu.make_async_copy(source, mine.at[pl.ds(at, rows)], local_sem.at[place])
        for place, (source, at, rows) in enumerate(own)
    ]
    token_load = pltpu.make_async_copy(tokens_in, tokens, token_sem)
    for load in loads:
        load.start()
    token_load.start()
    barrier = pltpu.get_barrier_semaphore()
    for peer in ("x", "y", "c", "zp", "zo", "far"):
        pl.semaphore_signal(barrier, inc=1, device_id=to[peer], device_id_type=MESH)
    pl.semaphore_wait(barrier, 6)
    for load in loads:
        load.wait()
    now()

    total_rows, width = tokens.shape
    blocks = total_rows // ROWS

    def norm_rows(source, gain_row):
        gain = gain_ref[gain_row:gain_row + 1, :]

        def body(step, carry):
            rows = pl.ds(pl.multiple_of(step * 128, 128), 128)
            wide = source[rows, :].astype(jnp.float32)
            square = jnp.mean(wide * wide, axis=-1, keepdims=True)
            normed[rows, :] = (wide * lax.rsqrt(square + 1e-05) * gain).astype(jnp.bfloat16)
            return carry
        lax.fori_loop(0, total_rows // 128, body, 0)

    token_load.wait()
    now()
    norm_rows(tokens, 0)
    now()
    lane = lax.broadcasted_iota(jnp.int32, (1, WIDE), 1)
    half_head = HEAD_DIM // 2
    times = jnp.broadcast_to(time_ref[...].astype(jnp.float32), (WIDE, total_rows)).T
    freq = jnp.exp(lax.rem(lane, half_head).astype(jnp.float32) * (-math.log(10000.0) / half_head))
    front = lax.rem(lane, HEAD_DIM) < half_head
    angle = times * freq
    cosine[...] = jnp.cos(angle)
    sine[...] = jnp.where(front, -1.0, 1.0) * jnp.sin(angle)
    variates = jnp.broadcast_to(variate_ref[...].astype(jnp.float32), (WIDE, total_rows)).T
    spare = lax.rem(lane, HEAD_DIM)
    number = lax.rem(spare, 16).astype(jnp.float32)
    third = spare // 16
    kinds[...] = jnp.where(
        jnp.logical_and(variates == number, third < 3), 1.0, 0.0
    ).astype(jnp.bfloat16)
    samples = sample_ref[...].astype(jnp.float32)
    for quarter in range(total_rows // WIDE):
        rows = slice(quarter * WIDE, (quarter + 1) * WIDE)
        column = jnp.broadcast_to(samples[:, rows], (WIDE, WIDE)).T
        for piece in range(L // WIDE):
            base = quarter * WIDE // L * L + piece * WIDE
            other = samples[:, base:base + WIDE]
            mask[rows, piece * WIDE:(piece + 1) * WIDE] = jnp.where(column == other, 0.0, -1e30)

    left = lane < HEAD_DIM

    def rows_of(at, count, index):
        return jnp.concatenate(
            [
                weights[a, b, c, index, pl.ds(at, count), :]
                for a in range(2) for b in range(2) for c in range(2)
            ],
            axis=0,
        )

    def rotated(raw, factor):
        swapped = jnp.where(
            front, pltpu.roll(raw, WIDE - half_head, 1), pltpu.roll(raw, half_head, 1)
        )
        return ((raw * cosine[...] + swapped * sine[...]) * factor).astype(jnp.bfloat16)

    def project(half, at, kind, held, run, base):
        def body(step, carry):
            run(base + step)
            weight = jnp.concatenate(
                [rows_of(at, width // 8, step * 2), rows_of(at, width // 8, step * 2 + 1)], axis=1
            )
            raw = jnp.dot(normed[...], weight, preferred_element_type=jnp.float32)
            for group in range(2):
                piece = raw[:, group * WIDE:(group + 1) * WIDE]
                if kind == 0:
                    piece = rotated(piece, HEAD_DIM ** -0.5 * LOG2E)
                elif kind == 1:
                    piece = rotated(piece, 1.0)
                else:
                    piece = piece.astype(jnp.bfloat16)
                held[(step * 2 + group) * HALVES + half] = piece
            return carry
        lax.fori_loop(0, 2, body, 0)

    def attend(half, run):
        def body(step, carry):
            run(step)
            pair = step // blocks * HALVES + half
            block = lax.rem(step, blocks)
            rows = pl.ds(pl.multiple_of(block * ROWS, ROWS), ROWS)
            span = pl.ds(pl.multiple_of((block * ROWS) // L * L, L), L)
            both = queries[pair, rows, :]
            key_rows = keys[pair, span, :]
            value_rows = values[pair, span, :]
            own_kinds = kinds[rows, :]
            other_kinds = kinds[span, :]
            one = jnp.ones((), jnp.bfloat16)
            mixed = []
            for side in range(2):
                head = pair * 2 + side
                chosen = left if side == 0 else jnp.logical_not(left)
                gap = jnp.full((1, WIDE), (bias_ref[0, head] - bias_ref[1, head]) * LOG2E, jnp.float32)
                first = gap.astype(jnp.bfloat16).astype(jnp.float32)
                second = (gap - first).astype(jnp.bfloat16).astype(jnp.float32)
                parts = jnp.where(third == 0, first, jnp.where(third == 1, second, gap - first - second))
                query = jnp.where(chosen, both, own_kinds * parts.astype(jnp.bfloat16))
                key = jnp.where(chosen, key_rows, other_kinds)
                value = jnp.where(chosen, value_rows, one)
                scores = lax.dot_general(
                    query, key, (((1,), (1,)), ((), ())), preferred_element_type=jnp.float32
                )
                scores = scores + mask[rows, :]
                top = jnp.max(scores, axis=1, keepdims=True)
                expo = jnp.exp2(scores - top).astype(jnp.bfloat16)
                mixed.append(jnp.dot(expo, value, preferred_element_type=jnp.float32))
            amount = jnp.where(left, mixed[0], mixed[1])
            share = pltpu.roll(jnp.where(left, mixed[1], mixed[0]), HEAD_DIM, 1)
            lanes = pl.ds(pl.multiple_of(pair * WIDE, WIDE), WIDE)
            attended[rows, lanes] = (amount / share).astype(jnp.bfloat16)
            return carry
        lax.fori_loop(0, width // WIDE // HALVES * blocks, body, 0)

    for half in range(HALVES):
        run = steps(6)
        for kind, held in enumerate((queries, keys, values)):
            project(half, spans[half * 3 + kind][0], kind, held, run, kind * 2)
        attend(half, steps(width // WIDE // HALVES * blocks))

    def columns_of(at, count, side_y, side_x):
        return jnp.concatenate(
            [
                jnp.concatenate(
                    [weights[side_y, side_x, c, index, pl.ds(at, count), :] for c in range(2)], axis=1
                )
                for index in range(LAYOUT[1])
            ],
            axis=0,
        )

    slab = 2 * WIDE
    out_at = spans[HALVES * 3][0]
    out_events = steps(4)

    def out_step(step, carry):
        out_events(step)
        lanes = pl.ds(pl.multiple_of(step * slab, slab), slab)
        weight = columns_of(out_at, width // LAYOUT[1], step // 2, lax.rem(step, 2))
        mixed = jnp.dot(attended[...], weight, preferred_element_type=jnp.float32)
        wide = (tokens[:, lanes].astype(jnp.float32) + mixed).astype(jnp.bfloat16)
        residual[:, lanes] = wide
        total[:, lanes] = wide.astype(jnp.float32)
        return carry
    lax.fori_loop(0, 4, out_step, 0)
    now()
    norm_rows(residual, 1)

    def hidden_weight(at):
        return jnp.concatenate(
            [
                jnp.concatenate(
                    [
                        weights[a, b, c, index, pl.ds(at, part), :]
                        for a in range(2) for b in range(2) for c in range(2)
                    ],
                    axis=1,
                )
                for index in range(LAYOUT[1])
            ],
            axis=0,
        )

    def against(at):
        return lax.dot_general(
            normed[...], hidden_weight(at), (((1,), (1,)), ((), ())),
            preferred_element_type=jnp.float32,
        )

    ff_at = spans[HALVES * 3 + 2][0]
    ff_events = steps(FF_PARTS * 4)

    def ff_step(index, carry):
        at = ff_at + index * (3 * part)
        at = pl.multiple_of(at, 16)
        ff_events(index * 4)
        gate[...] = against(at)
        ff_events(index * 4 + 1)
        up = against(pl.multiple_of(at + part, 16))
        opened = gate[...]
        hidden[...] = (opened / (1.0 + jnp.exp(-opened)) * up).astype(jnp.bfloat16)
        for pair in range(2):
            ff_events(index * 4 + 2 + pair)
            for side in range(2):
                lanes = slice((pair * 2 + side) * slab, (pair * 2 + side + 1) * slab)
                weight = columns_of(pl.multiple_of(at + 2 * part, 16), part, pair, side)
                fresh = total[:, lanes] + jnp.dot(
                    hidden[...], weight, preferred_element_type=jnp.float32
                )
                total[:, lanes] = fresh
        return carry
    lax.fori_loop(0, FF_PARTS, ff_step, 0)
    for piece in range(4):
        lanes = slice(piece * slab, (piece + 1) * slab)
        final_ref[:, lanes] = total[:, lanes].astype(jnp.bfloat16)
    all_sent()


def spans_of(qkv, out, ffn):
    found, row = [], 0
    for rows in [qkv.shape[1]] * (3 * HALVES) + [out.shape[0] // 2] * 2 + [ffn.shape[1] // FF_PARTS] * (3 * FF_PARTS):
        found.append((row, rows))
        row += rows
    return tuple(found), row


def fused(
    tokens, norm_gain, qkv_weight, out_weight, variate_bias, ffn_weight, down_weight,
    sample_ids, variate_ids, time_ids,
):
    rows, width = tokens.shape
    ffn = jnp.swapaxes(ffn_weight, 1, 2)
    spans, depth = spans_of(qkv_weight, out_weight, ffn)
    vmem = pl.BlockSpec(memory_space=pltpu.VMEM)
    anywhere = pl.BlockSpec(memory_space=pl.ANY)
    per_pair = pltpu.VMEM((width // WIDE, rows, WIDE), jnp.bfloat16)
    flat = pltpu.VMEM((rows, width), jnp.bfloat16)
    strip = pltpu.VMEM((rows, WIDE), jnp.float32)
    ff_wide = LAYOUT[1] * ffn.shape[1] // FF_PARTS
    copies = len(KINDS) * len(SLOTS)
    return pl.pallas_call(
        functools.partial(layer_kernel, spans),
        out_shape=pltpu.VMEM((rows, width), jnp.bfloat16),
        in_specs=[pl.BlockSpec(memory_space=pltpu.SMEM)] + [vmem] * 4 + [anywhere] * 5,
        out_specs=pl.BlockSpec(memory_space=pltpu.VMEM),
        scratch_shapes=[
            pltpu.VMEM((2, 2, 2, LAYOUT[1], depth, WIDE), jnp.bfloat16),
            flat, flat, per_pair, per_pair, per_pair, flat, flat,
            pltpu.VMEM((rows, ff_wide), jnp.float32),
            pltpu.VMEM((rows, ff_wide), jnp.bfloat16),
            pltpu.VMEM((rows, width), jnp.float32),
            strip, strip, pltpu.VMEM((rows, WIDE), jnp.bfloat16),
            pltpu.VMEM((rows, L), jnp.float32),
            pltpu.SemaphoreType.DMA((copies,)),
            pltpu.SemaphoreType.DMA((copies,)),
            pltpu.SemaphoreType.DMA((3 * HALVES + 1 + 3 * FF_PARTS,)),
            pltpu.SemaphoreType.DMA(()),
        ],
        compiler_params=pltpu.CompilerParams(
            collective_id=0, has_side_effects=True, vmem_limit_bytes=62 * 1024 * 1024
        ),
    )(
        variate_bias, norm_gain, sample_ids.reshape(1, -1), variate_ids.reshape(1, -1),
        time_ids.reshape(1, -1), tokens, qkv_weight, out_weight, ffn, down_weight,
    )


def solution(mesh):
    body = fused if (mesh.shape["dp"], mesh.shape["mp"]) == LAYOUT else local
    return jax.shard_map(
        body,
        mesh=mesh,
        in_specs=(
            P(("dp", "mp"), None),
            P(),
            P(None, "dp", "mp"),
            P("mp", "dp"),
            P(),
            P(None, "dp", "mp"),
            P("mp", "dp"),
            P(("dp", "mp")),
            P(("dp", "mp")),
            P(("dp", "mp")),
        ),
        out_specs=P(("dp", "mp"), None),
        check_vma=False,
    )
```

```python
import functools
import math

import jax
import jax.numpy as jnp
from jax import lax
from jax.experimental import pallas as pl
from jax.experimental.pallas import tpu as pltpu
from jax.sharding import PartitionSpec as P

HEAD_DIM = 64
L = 512


def rms_norm(values, gain):
    wide = values.astype(jnp.float32)
    square = jnp.mean(wide * wide, axis=-1, keepdims=True)
    return (wide * lax.rsqrt(square + 1e-05) * gain[None, :]).astype(jnp.bfloat16)


def rotate(values, times):
    half = values.shape[-1] // 2
    freq = 10000.0 ** (-jnp.arange(half, dtype=jnp.float32) / half)
    angle = times.astype(jnp.float32)[:, None] * freq[None, :]
    cosine = jnp.cos(angle)[:, None, :]
    sine = jnp.sin(angle)[:, None, :]
    first = values[..., :half]
    second = values[..., half:]
    return jnp.concatenate(
        [first * cosine - second * sine, first * sine + second * cosine], axis=-1
    )


def rotated(raw, times):
    row_total, local_width = raw.shape
    turned = rotate(raw.reshape(row_total, local_width // HEAD_DIM, HEAD_DIM), times)
    return turned.reshape(row_total, local_width).astype(jnp.bfloat16)


def attend(queries, keys_rot, values, samples, variates, bias):
    row_total, local_width = queries.shape
    heads_here = local_width // HEAD_DIM
    count = row_total // L

    def one_sequence(args):
        qs, ks, vs, sample_row, variate_row = args
        scores = jnp.einsum(
            "qhd,khd->hqk", qs, ks, preferred_element_type=jnp.float32
        ) * HEAD_DIM ** (-0.5)
        same = variate_row[:, None] == variate_row[None, :]
        scores = scores + jnp.where(same[None], bias[0][:, None, None], bias[1][:, None, None])
        scores = jnp.where((sample_row[:, None] == sample_row[None, :])[None], scores, -1e30)
        top = jnp.max(scores, axis=2, keepdims=True)
        expo = jnp.exp(scores - top)
        weights = (expo / jnp.sum(expo, axis=2, keepdims=True)).astype(jnp.bfloat16)
        return jnp.einsum("hqk,khd->qhd", weights, vs, preferred_element_type=jnp.float32).astype(
            jnp.bfloat16
        )

    shape = (count, L, heads_here, HEAD_DIM)
    result = lax.map(
        one_sequence,
        (
            queries.reshape(shape),
            keys_rot.reshape(shape),
            values.reshape(shape),
            samples.reshape(count, L),
            variates.reshape(count, L),
        ),
    )
    return result.reshape(row_total, local_width)


def local(
    tokens,
    norm_gain,
    qkv_weight,
    out_weight,
    variate_bias,
    ffn_weight,
    down_weight,
    sample_ids,
    variate_ids,
    time_ids,
):
    first_normed = rms_norm(tokens, norm_gain[0])
    wide_columns = lax.all_gather(qkv_weight, "mp", axis=2, tiled=True)
    columns = first_normed
    projected = jnp.einsum(
        "rc,jcd->jrd",
        columns,
        lax.all_gather(wide_columns, "dp", axis=1, tiled=True),
        preferred_element_type=jnp.float32,
    )
    queries = rotated(projected[0], time_ids)
    keys_rot = rotated(projected[1], time_ids)
    values = projected[2].astype(jnp.bfloat16)
    back_rows = attend(queries, keys_rot, values, sample_ids, variate_ids, variate_bias)
    out_rows = lax.all_gather(out_weight, "mp", axis=0, tiled=True)
    mixed = jnp.dot(
        back_rows,
        lax.all_gather(out_rows, "dp", axis=1, tiled=True),
        preferred_element_type=jnp.float32,
    )
    residual = (tokens.astype(jnp.float32) + mixed).astype(jnp.bfloat16)
    second_normed = rms_norm(residual, norm_gain[1])
    ffn_columns = lax.all_gather(ffn_weight, "mp", axis=2, tiled=True)
    columns = second_normed
    gate_up = jnp.einsum(
        "rc,jcf->jrf",
        columns,
        lax.all_gather(ffn_columns, "dp", axis=1, tiled=True),
        preferred_element_type=jnp.float32,
    )
    hidden = (jax.nn.silu(gate_up[0]) * gate_up[1]).astype(jnp.bfloat16)
    down_full = lax.all_gather(down_weight, "mp", axis=0, tiled=True)
    feed = jnp.dot(
        hidden,
        lax.all_gather(down_full, "dp", axis=1, tiled=True),
        preferred_element_type=jnp.float32,
    )
    return (residual.astype(jnp.float32) + feed).astype(jnp.bfloat16)

MESH = pl.DeviceIdType.MESH
WIDE = 2 * HEAD_DIM
ROWS = 512
LAYOUT = (2 ** 3, 2 ** 2)
HALVES = 2
FF_PARTS = 4
LOG2E = math.log2(math.e)
SLOTS = ("zp", "zoE", "zoM", "zf", "p1", "p2", "a1", "a2")
KINDS = "AAAAAAAAAAABABABABAA"
LEADS = "xyxyxxyyyxxxyyxxyyxy"
PLAN = (
    ((1, 0), (13, 0), (0, 0), (11, 0), (3, 0), (2, 0), (7, 0), (17, 0), (5, 0), (15, 0),),
    ((1, 1), (11, 1), (15, 1), (17, 1), (0, 1), (13, 1), (3, 1), (1, 2), (2, 1), (0, 2), (7, 1), (6, 0), (3, 2), (9, 0),),
    ((5, 1), (10, 0), (4, 0), (2, 2), (7, 2), (12, 0), (8, 0), (6, 1), (16, 0), (1, 3),),
    ((0, 3), (5, 2), (4, 1), (12, 1), (6, 2), (19, 0), (3, 3), (4, 2), (18, 0), (14, 0), (8, 1), (2, 3), (8, 2), (10, 1), (9, 1), (0, 4), (3, 4), (16, 1), (7, 3), (14, 1), (12, 2), (13, 2), (6, 3), (18, 1), (5, 3), (9, 2), (14, 2), (16, 2), (11, 2), (15, 2), (10, 2), (19, 1), (4, 3), (8, 3), (7, 4), (6, 4), (2, 4), (1, 4), (2, 5), (1, 5), (6, 5), (18, 2), (0, 5),),
    ((9, 3), (13, 3), (5, 4),),
    (),
    (),
    (),
    (),
    (),
    ((19, 2),),
    (),
    ((4, 4), (12, 3), (10, 3), (11, 3),),
    ((13, 4), (15, 3), (14, 3), (5, 5), (17, 2), (3, 5),),
    (),
    ((13, 5), (4, 5),),
    (),
    (),
    (),
    ((8, 4), (7, 5), (16, 3), (9, 4),),
    (),
    (),
    ((18, 3), (8, 5),),
    (),
    (),
    (),
    (),
    (),
    (),
    ((10, 4), (12, 4), (11, 4), (19, 3), (10, 5), (9, 5), (17, 3),),
    (),
    (),
    ((11, 5), (15, 4),),
    ((14, 4), (16, 4), (12, 5),),
    (),
    ((14, 5), (15, 5),),
    (),
    (),
    ((17, 4), (16, 5),),
    (),
    ((18, 4), (19, 4), (17, 5),),
    ((18, 5),),
    ((19, 5),),
    (),
)


def stages(kind, lead):
    other = "y" if lead == "x" else "x"
    if kind == "A":
        return [
            ((), (("zp", "z"), ("zo", "z"))),
            (("ZM",), (("zf", "z"),)),
            (("ZP", "ZF"), (("p1", lead),)),
            (("p1",), (("p2", other), ("a1", "c"))),
            (("p2",), (("a2", "c"),)),
            (("a1", "a2"), ()),
        ]
    return [
        ((), (("p1", lead),)),
        (("p1",), (("p2", other),)),
        (("p2",), (("zp", "z"), ("zo", "z"))),
        (("ZM",), (("zf", "z"),)),
        (("ZP", "ZF"), (("a2", "c"),)),
        (("a2",), ()),
    ]


def layer_kernel(
    spans,
    bias_ref, gain_in, sample_in, variate_in, time_in, tokens_in, qkv_in, out_in, ffn_in, down_in,
    final_ref,
    weights, tokens, normed, queries, keys, values, attended, residual, gate, hidden, total,
    cosine, sine, kinds, mask, gain_ref, sample_ref, variate_ref, time_ref,
    send_sem, recv_sem, local_sem, input_sem,
):
    dp = lax.axis_index("dp")
    z = lax.axis_index("mp")
    core = lax.rem(dp, 2)
    x = lax.rem(dp // 2, 2)
    y = dp // 4
    whole = slice(None)
    is_mid = jnp.logical_or(z == 1, z == 2)
    low = z < 2
    partner_z = z + 1 - 2 * lax.rem(z, 2)
    far_mid = jnp.where(low, 2, 1)
    far_end = jnp.where(low, 3, 0)
    far_half = pl.ds(jnp.where(low, 2, 0), 2)
    to = {
        "x": {"dp": (y * 2 + 1 - x) * 2 + core, "mp": z},
        "y": {"dp": ((1 - y) * 2 + x) * 2 + core, "mp": z},
        "c": {"dp": (y * 2 + x) * 2 + 1 - core, "mp": z},
        "zp": {"dp": dp, "mp": partner_z},
        "zo": {"dp": dp, "mp": far_mid},
        "far": {"dp": dp, "mp": far_end},
    }
    to["zf"] = to["zp"]

    def region(chunk, name):
        kind, lead = KINDS[chunk], LEADS[chunk]
        if name in ("zp", "zo"):
            head = (y, x, core, z) if kind == "A" else (whole, whole, core, z)
        elif name == "zf":
            head = (y, x, core, far_half) if kind == "A" else (whole, whole, core, far_half)
        elif name == "p1":
            head = (y, x, core, whole) if kind == "A" else (y, x, core, z)
        else:
            cut = slice(None) if kind == "A" else z
            if name == "p2":
                head = ((y, whole) if lead == "x" else (whole, x)) + (core, cut)
            elif name == "a1":
                head = ((y, whole) if lead == "x" else (whole, x)) + (core, whole)
            elif kind == "A":
                head = ((1 - y, whole) if lead == "x" else (whole, 1 - x)) + (core, whole)
            else:
                head = (whole, whole, core, whole)
        start, rows = spans[chunk]
        return head + (pl.ds(start, rows),)

    def copy(chunk, name, target, landing=None):
        part = weights.at[region(chunk, name)]
        slot = chunk * len(SLOTS)
        if name == "zo" and landing is None:
            slot = slot + jnp.where(is_mid, SLOTS.index("zoM"), SLOTS.index("zoE"))
        else:
            slot = slot + SLOTS.index(landing or name)
        return pltpu.make_async_remote_copy(
            src_ref=part, dst_ref=part, send_sem=send_sem.at[slot], recv_sem=recv_sem.at[slot],
            device_id=target, device_id_type=MESH,
        )

    def axis_of(chunk, name):
        lead = LEADS[chunk]
        other = "y" if lead == "x" else "x"
        return {"p1": lead, "p2": other, "a1": "c", "a2": "c"}.get(name, name)

    def wait_for(chunk, mark):
        if mark == "ZM":
            @pl.when(is_mid)
            def _():
                copy(chunk, "zo", to["zo"], "zoE").wait_recv()
                copy(chunk, "zo", to["zo"], "zoM").wait_recv()
        elif mark == "ZP":
            copy(chunk, "zp", to["zp"]).wait_recv()
        elif mark == "ZF":
            @pl.when(jnp.logical_not(is_mid))
            def _():
                copy(chunk, "zf", to["zf"]).wait_recv()
        else:
            copy(chunk, mark, to[axis_of(chunk, mark)]).wait_recv()

    def event(chunk, stage):
        waits, sends = stages(KINDS[chunk], LEADS[chunk])[stage]
        for mark in waits:
            wait_for(chunk, mark)
        for name, _ in sends:
            begin = copy(chunk, name, to[axis_of(chunk, name)]).start
            if name == "zf":
                pl.when(is_mid)(begin)
            else:
                begin()

    def all_sent():
        for chunk in range(len(KINDS)):
            for _, sends in stages(KINDS[chunk], LEADS[chunk]):
                for name, _ in sends:
                    finish = copy(chunk, name, to[axis_of(chunk, name)]).wait_send
                    if name == "zf":
                        pl.when(is_mid)(finish)
                    else:
                        finish()

    cursor = [0]

    def now():
        for item in PLAN[cursor[0]]:
            event(*item)
        cursor[0] += 1

    def steps(count):
        plan = PLAN[cursor[0]:cursor[0] + count]
        cursor[0] += count

        def run(step):
            for place, items in enumerate(plan):
                if items:
                    @pl.when(step == place)
                    def _():
                        for item in items:
                            event(*item)
        return run

    mine = weights.at[y, x, core, z]
    own = []
    row = 0
    for half in range(HALVES):
        for kind in range(3):
            own.append((qkv_in.at[kind, :, pl.ds(half * WIDE, WIDE)], row, qkv_in.shape[1]))
            row += qkv_in.shape[1]
    own.append((out_in, row, out_in.shape[0]))
    row += out_in.shape[0]
    part = ffn_in.shape[1] // FF_PARTS
    for index in range(FF_PARTS):
        for source in (ffn_in.at[0], ffn_in.at[1], down_in):
            own.append((source.at[pl.ds(index * part, part)], row, part))
            row += part
    loads = [
        pltpu.make_async_copy(source, mine.at[pl.ds(at, rows)], local_sem.at[place])
        for place, (source, at, rows) in enumerate(own)
    ]
    inputs = [
        pltpu.make_async_copy(source, held, input_sem.at[place])
        for place, (source, held) in enumerate(
            (
                (tokens_in, tokens), (gain_in, gain_ref), (sample_in, sample_ref),
                (variate_in, variate_ref), (time_in, time_ref),
            )
        )
    ]
    for load in loads:
        load.start()
    barrier = pltpu.get_barrier_semaphore()
    for peer in ("x", "y", "c", "zp", "zo", "far"):
        pl.semaphore_signal(barrier, inc=1, device_id=to[peer], device_id_type=MESH)
    pl.semaphore_wait(barrier, 6)
    for load in inputs:
        load.start()
    for load in loads:
        load.wait()
    now()

    total_rows, width = tokens.shape
    blocks = total_rows // ROWS

    def norm_rows(source, gain_row):
        gain = gain_ref[gain_row:gain_row + 1, :]

        def body(step, carry):
            rows = pl.ds(pl.multiple_of(step * 128, 128), 128)
            wide = source[rows, :].astype(jnp.float32)
            square = jnp.mean(wide * wide, axis=-1, keepdims=True)
            normed[rows, :] = (wide * lax.rsqrt(square + 1e-05) * gain).astype(jnp.bfloat16)
            return carry
        lax.fori_loop(0, total_rows // 128, body, 0)

    for load in inputs:
        load.wait()
    now()
    norm_rows(tokens, 0)
    now()
    lane = lax.broadcasted_iota(jnp.int32, (1, WIDE), 1)
    half_head = HEAD_DIM // 2
    times = jnp.broadcast_to(time_ref[...].astype(jnp.float32), (WIDE, total_rows)).T
    freq = jnp.exp(lax.rem(lane, half_head).astype(jnp.float32) * (-math.log(10000.0) / half_head))
    front = lax.rem(lane, HEAD_DIM) < half_head
    angle = times * freq
    cosine[...] = jnp.cos(angle)
    sine[...] = jnp.where(front, -1.0, 1.0) * jnp.sin(angle)
    variates = jnp.broadcast_to(variate_ref[...].astype(jnp.float32), (WIDE, total_rows)).T
    spare = lax.rem(lane, HEAD_DIM)
    number = lax.rem(spare, 16).astype(jnp.float32)
    third = spare // 16
    kinds[...] = jnp.where(
        jnp.logical_and(variates == number, third < 3), 1.0, 0.0
    ).astype(jnp.bfloat16)
    samples = sample_ref[...].astype(jnp.float32)
    for quarter in range(total_rows // WIDE):
        rows = slice(quarter * WIDE, (quarter + 1) * WIDE)
        column = jnp.broadcast_to(samples[:, rows], (WIDE, WIDE)).T
        for piece in range(L // WIDE):
            base = quarter * WIDE // L * L + piece * WIDE
            other = samples[:, base:base + WIDE]
            mask[rows, piece * WIDE:(piece + 1) * WIDE] = jnp.where(column == other, 0.0, -1e30)

    left = lane < HEAD_DIM

    def rows_of(at, count, index):
        return jnp.concatenate(
            [
                weights[a, b, c, index, pl.ds(at, count), :]
                for a in range(2) for b in range(2) for c in range(2)
            ],
            axis=0,
        )

    def rotated(raw, factor):
        swapped = jnp.where(
            front, pltpu.roll(raw, WIDE - half_head, 1), pltpu.roll(raw, half_head, 1)
        )
        return ((raw * cosine[...] + swapped * sine[...]) * factor).astype(jnp.bfloat16)

    def project(half, at, kind, held, run, base):
        def body(step, carry):
            run(base + step)
            weight = jnp.concatenate(
                [rows_of(at, width // 8, step * 2), rows_of(at, width // 8, step * 2 + 1)], axis=1
            )
            raw = jnp.dot(normed[...], weight, preferred_element_type=jnp.float32)
            for group in range(2):
                piece = raw[:, group * WIDE:(group + 1) * WIDE]
                if kind == 0:
                    piece = rotated(piece, HEAD_DIM ** -0.5 * LOG2E)
                elif kind == 1:
                    piece = rotated(piece, 1.0)
                else:
                    piece = piece.astype(jnp.bfloat16)
                held[(step * 2 + group) * HALVES + half] = piece
            return carry
        lax.fori_loop(0, 2, body, 0)

    def attend(half, run):
        def body(step, carry):
            run(step)
            pair = step // blocks * HALVES + half
            block = lax.rem(step, blocks)
            rows = pl.ds(pl.multiple_of(block * ROWS, ROWS), ROWS)
            span = pl.ds(pl.multiple_of((block * ROWS) // L * L, L), L)
            both = queries[pair, rows, :]
            key_rows = keys[pair, span, :]
            value_rows = values[pair, span, :]
            own_kinds = kinds[rows, :]
            other_kinds = kinds[span, :]
            one = jnp.ones((), jnp.bfloat16)
            mixed = []
            for side in range(2):
                head = pair * 2 + side
                chosen = left if side == 0 else jnp.logical_not(left)
                gap = jnp.full((1, WIDE), (bias_ref[0, head] - bias_ref[1, head]) * LOG2E, jnp.float32)
                first = gap.astype(jnp.bfloat16).astype(jnp.float32)
                second = (gap - first).astype(jnp.bfloat16).astype(jnp.float32)
                parts = jnp.where(third == 0, first, jnp.where(third == 1, second, gap - first - second))
                query = jnp.where(chosen, both, own_kinds * parts.astype(jnp.bfloat16))
                key = jnp.where(chosen, key_rows, other_kinds)
                value = jnp.where(chosen, value_rows, one)
                scores = lax.dot_general(
                    query, key, (((1,), (1,)), ((), ())), preferred_element_type=jnp.float32
                )
                scores = scores + mask[rows, :]
                top = jnp.max(scores, axis=1, keepdims=True)
                expo = jnp.exp2(scores - top).astype(jnp.bfloat16)
                mixed.append(jnp.dot(expo, value, preferred_element_type=jnp.float32))
            amount = jnp.where(left, mixed[0], mixed[1])
            share = pltpu.roll(jnp.where(left, mixed[1], mixed[0]), HEAD_DIM, 1)
            lanes = pl.ds(pl.multiple_of(pair * WIDE, WIDE), WIDE)
            attended[rows, lanes] = (amount / share).astype(jnp.bfloat16)
            return carry
        lax.fori_loop(0, width // WIDE // HALVES * blocks, body, 0)

    for half in range(HALVES):
        run = steps(6)
        for kind, held in enumerate((queries, keys, values)):
            project(half, spans[half * 3 + kind][0], kind, held, run, kind * 2)
        attend(half, steps(width // WIDE // HALVES * blocks))

    def columns_of(at, count, side_y, side_x):
        return jnp.concatenate(
            [
                jnp.concatenate(
                    [weights[side_y, side_x, c, index, pl.ds(at, count), :] for c in range(2)], axis=1
                )
                for index in range(LAYOUT[1])
            ],
            axis=0,
        )

    slab = 2 * WIDE
    out_at = spans[HALVES * 3][0]
    out_events = steps(4)

    def out_step(step, carry):
        out_events(step)
        lanes = pl.ds(pl.multiple_of(step * slab, slab), slab)
        weight = columns_of(out_at, width // LAYOUT[1], step // 2, lax.rem(step, 2))
        mixed = jnp.dot(attended[...], weight, preferred_element_type=jnp.float32)
        wide = (tokens[:, lanes].astype(jnp.float32) + mixed).astype(jnp.bfloat16)
        residual[:, lanes] = wide
        total[:, lanes] = wide.astype(jnp.float32)
        return carry
    lax.fori_loop(0, 4, out_step, 0)
    now()
    norm_rows(residual, 1)

    def hidden_weight(at):
        return jnp.concatenate(
            [
                jnp.concatenate(
                    [
                        weights[a, b, c, index, pl.ds(at, part), :]
                        for a in range(2) for b in range(2) for c in range(2)
                    ],
                    axis=1,
                )
                for index in range(LAYOUT[1])
            ],
            axis=0,
        )

    def against(at):
        return lax.dot_general(
            normed[...], hidden_weight(at), (((1,), (1,)), ((), ())),
            preferred_element_type=jnp.float32,
        )

    ff_at = spans[HALVES * 3 + 2][0]
    ff_events = steps(FF_PARTS * 4)

    def ff_step(index, carry):
        at = ff_at + index * (3 * part)
        at = pl.multiple_of(at, 16)
        ff_events(index * 4)
        gate[...] = against(at)
        ff_events(index * 4 + 1)
        up = against(pl.multiple_of(at + part, 16))
        opened = gate[...]
        hidden[...] = (opened / (1.0 + jnp.exp(-opened)) * up).astype(jnp.bfloat16)
        for pair in range(2):
            ff_events(index * 4 + 2 + pair)
            for side in range(2):
                lanes = slice((pair * 2 + side) * slab, (pair * 2 + side + 1) * slab)
                weight = columns_of(pl.multiple_of(at + 2 * part, 16), part, pair, side)
                fresh = total[:, lanes] + jnp.dot(
                    hidden[...], weight, preferred_element_type=jnp.float32
                )
                total[:, lanes] = fresh
                final_ref[:, lanes] = fresh.astype(jnp.bfloat16)
        return carry
    lax.fori_loop(0, FF_PARTS, ff_step, 0)
    all_sent()


def spans_of(qkv, out, ffn):
    found, row = [], 0
    for rows in [qkv.shape[1]] * (3 * HALVES) + [out.shape[0] // 2] * 2 + [ffn.shape[1] // FF_PARTS] * (3 * FF_PARTS):
        found.append((row, rows))
        row += rows
    return tuple(found), row


def fused(
    tokens, norm_gain, qkv_weight, out_weight, variate_bias, ffn_weight, down_weight,
    sample_ids, variate_ids, time_ids,
):
    rows, width = tokens.shape
    ffn = jnp.swapaxes(ffn_weight, 1, 2)
    spans, depth = spans_of(qkv_weight, out_weight, ffn)
    anywhere = pl.BlockSpec(memory_space=pl.ANY)
    per_pair = pltpu.VMEM((width // WIDE, rows, WIDE), jnp.bfloat16)
    flat = pltpu.VMEM((rows, width), jnp.bfloat16)
    strip = pltpu.VMEM((rows, WIDE), jnp.float32)
    ff_wide = LAYOUT[1] * ffn.shape[1] // FF_PARTS
    copies = len(KINDS) * len(SLOTS)
    return pl.pallas_call(
        functools.partial(layer_kernel, spans),
        out_shape=pltpu.VMEM((rows, width), jnp.bfloat16),
        in_specs=[pl.BlockSpec(memory_space=pltpu.SMEM)] + [anywhere] * 9,
        out_specs=pl.BlockSpec(memory_space=pltpu.VMEM),
        scratch_shapes=[
            pltpu.VMEM((2, 2, 2, LAYOUT[1], depth, WIDE), jnp.bfloat16),
            flat, flat, per_pair, per_pair, per_pair, flat, flat,
            pltpu.VMEM((rows, ff_wide), jnp.float32),
            pltpu.VMEM((rows, ff_wide), jnp.bfloat16),
            pltpu.VMEM((rows, width), jnp.float32),
            strip, strip, pltpu.VMEM((rows, WIDE), jnp.bfloat16),
            pltpu.VMEM((rows, L), jnp.float32),
            pltpu.VMEM(norm_gain.shape, jnp.float32),
        ] + [pltpu.VMEM((1, rows), jnp.int32)] * 3 + [
            pltpu.SemaphoreType.DMA((copies,)),
            pltpu.SemaphoreType.DMA((copies,)),
            pltpu.SemaphoreType.DMA((3 * HALVES + 1 + 3 * FF_PARTS,)),
            pltpu.SemaphoreType.DMA((5,)),
        ],
        compiler_params=pltpu.CompilerParams(
            collective_id=0, has_side_effects=True, vmem_limit_bytes=62 * 1024 * 1024
        ),
    )(
        variate_bias, norm_gain, sample_ids.reshape(1, -1), variate_ids.reshape(1, -1),
        time_ids.reshape(1, -1), tokens, qkv_weight, out_weight, ffn, down_weight,
    )


def solution(mesh):
    body = fused if (mesh.shape["dp"], mesh.shape["mp"]) == LAYOUT else local
    return jax.shard_map(
        body,
        mesh=mesh,
        in_specs=(
            P(("dp", "mp"), None),
            P(),
            P(None, "dp", "mp"),
            P("mp", "dp"),
            P(),
            P(None, "dp", "mp"),
            P("mp", "dp"),
            P(("dp", "mp")),
            P(("dp", "mp")),
            P(("dp", "mp")),
        ),
        out_specs=P(("dp", "mp"), None),
        check_vma=False,
    )
```
